32 devices in a mesh: expert: 16 (over z, y, x), store: 2 (over core).
Axes of the slice: x: 2, y: 2, z: 4, core: 2. Of those that a mesh axis runs over, the one named last changes fastest.
Arguments:
- tokens: bfloat16 [4096, 2048], P(('expert', 'store')), may hold values from -6 to 6
- chosen_expert_index: int32 [4096, 8], P(('expert', 'store')), may hold values from 0 to 15, all different within a row; in each aligned block of 128 rows (0 to 127, 128 to 255, ...) at most 72 rows name the same one
- router_weight_logits: float32 [4096, 8], P(('expert', 'store')), may hold values from 0.1 to 1
- token_tenant_index: int32 [4096], P(('expert', 'store')), may hold values from 0 to 1
- adapted: int32 [2, 16], P(None, 'expert'), may hold values 0 or 1
- gate_up_weight: bfloat16 [16, 2048, 768], P('expert', 'store'), may hold values from -0.125 to 0.125
- down_weight: bfloat16 [16, 384, 2048], P('expert', None, 'store'), may hold values from -0.3125 to 0.3125
- adapter_input_factors: bfloat16 [2, 16, 32, 2048], P('store', 'expert'), may hold values from -0.125 to 0.125
- adapter_output_factors: bfloat16 [2, 16, 32, 384], P('store', 'expert'), may hold values from -0.8984375 to 0.8984375
Outputs:
- mixed: bfloat16 [4096, 2048], P(('expert', 'store'))
The draws below stay inside these ranges and needn't reach their ends.
Inputs may be any that keep to these rules, and one draw needn't show every extreme that they name: `chosen_expert_index`: each row names 8 different experts; within the rows of one device no expert is named by more than 72 rows.
All inputs are finite; a program needn't handle non-finite values. No bound on the sum of `adapted` on one device may be relied on, other than what follows from the above.
Results may differ from the reference program's by a relative error of at most 0.006.
Values may be sent and summed in bfloat16 or wider, within the bound.
No kernel may reach another device: no remote copies, remote signals or barrier semaphores. Data moves between devices by JAX's collectives and lax.ppermute only.
A program may use at most 128 MiB of HBM per device.

```python
import math
import jax
import jax.numpy as jnp
import numpy as np
from jax import lax

MODEL_DIMENSION = 2048
EXPERT_HIDDEN = 384
ADAPTER_RANK = 16
TOPK = 8
TOK_DEV = 128
EXPERT_TOTAL = 16
CAP = 72
TENANT_TOTAL = 2
TOKENS = 4096


def touch_ends(drawn, key, smallest, top_value):
    dims = drawn.shape
    spot = [jax.random.randint(jax.random.fold_in(key, axis), (), 0, dims[axis]) for axis in range(len(dims))]
    drawn = drawn.at[tuple(spot)].set(smallest)
    longest = dims.index(max(dims))
    spot[longest] = (spot[longest] + 1) % dims[longest]
    return drawn.at[tuple(spot)].set(top_value)


def block_levels(key, extent, cuts, low, high):
    def one(dim, shards_of):
        heights = jax.random.uniform(jax.random.fold_in(jax.random.fold_in(key, 6), dim), (shards_of,), jnp.float32, low / len(cuts), high / len(cuts))
        return jnp.repeat(jnp.exp(heights), extent[dim] // shards_of).reshape((-1,) + (1,) * (len(extent) - dim - 1))

    loudness = one(*cuts[0])
    for cut in cuts[1:]:
        loudness = loudness * one(*cut)
    return loudness


def deal_out(key, own, number, rows, amount, top, bound, slope):
    order = jax.random.permutation(key, amount)
    crowded, usual = portions_of(amount, rows * top, bound, slope, True), portions_of(amount, rows * top, bound, slope, False)
    places = jnp.arange(amount)

    def named(tallies, turn):
        used = int((tallies > 0).sum())
        fixed = max(1, used // 4)
        moved = fixed + (places - fixed + turn * (used - fixed)) % max(1, amount - fixed)
        return jnp.zeros((amount,), jnp.int32).at[order[jnp.where(places < fixed, places, moved)]].set(jnp.asarray(tallies, jnp.int32))

    tallies = jnp.where(number % 4 == 0, named(crowded, number // 4), named(usual, number - number // 4 - 1))
    mixed = jax.random.permutation(jax.random.fold_in(own, 3), amount)
    giver, taker = mixed[0:amount // 2 * 2:2], mixed[1:amount // 2 * 2:2]
    margin = jnp.minimum(tallies[giver] - 1, bound - tallies[taker]) // 2
    margin = jnp.where((giver == order[0]) | (taker == order[0]) | (tallies[taker] == 0), 0, jnp.maximum(margin, 0))
    moved = jax.random.randint(jax.random.fold_in(own, 4), (amount // 2,), 0, 1 << 20) % (margin + 1)
    tallies = tallies.at[giver].add(-moved).at[taker].add(moved)
    items = jnp.searchsorted(jnp.cumsum(tallies), jnp.arange(rows * top), side="right").astype(jnp.int32)
    table = items.reshape(top, rows).T
    table = table[jax.random.permutation(jax.random.fold_in(own, 1), rows)]
    turn = jax.random.randint(jax.random.fold_in(own, 2), (rows, 1), 0, top)
    return jnp.take_along_axis(table, (jnp.arange(top)[None, :] + turn) % top, axis=1)


def portions_of(count, total, most, lean, full):
    loads = [(1 << 20) // math.isqrt(rank ** lean) + 1 for rank in range(1, count + 1)]
    largest = most if full else min(most, max(-(-total // count), total * loads[0] // sum(loads)))
    least = 1 if total - largest >= count - 1 else 0
    counts, surplus = [largest] + [least] * (count - 1), total - largest - least * (count - 1)
    while surplus > 0:
        movable = [i for i in range(1, count) if counts[i] < largest] or [i for i in range(1, count) if counts[i] < most]
        whole, budget = sum([loads[i] for i in movable]), surplus
        for i in movable:
            addition = min(most - counts[i], max(1, budget * loads[i] // whole), surplus)
            counts[i] = counts[i] + addition
            surplus = surplus - addition
    return np.array(counts)


def bell_draw(key, dims, spread, most, cuts=(), held_as=jnp.bfloat16):
    values = jax.random.normal(key, dims, jnp.float32) * spread
    if len(cuts) > 0:
        values = block_levels(key, dims, cuts, -0.22, 0.18) * values
    return jnp.clip(values, min=-most, max=most).astype(held_as)


def setup_inputs(seed: int = 0) -> dict:
    streams_of = jax.random.split(jax.random.key(seed), 10)
    tokens = bell_draw(streams_of[0], (TOKENS, MODEL_DIMENSION), 1.0, 6.0, ((0, 32),))
    chosen_expert_index_keys = jax.random.split(jax.random.fold_in(streams_of[1], 1), TOKENS // TOK_DEV)
    chosen_expert_index_turns = jax.random.permutation(jax.random.fold_in(streams_of[1], 3), TOKENS // TOK_DEV)
    chosen_expert_index = jax.vmap(lambda own, number: deal_out(jax.random.fold_in(streams_of[1], 2), own, number, TOK_DEV, EXPERT_TOTAL, TOPK, CAP, 2))(chosen_expert_index_keys, chosen_expert_index_turns).reshape((TOKENS, TOPK))
    router_weight_logits = jnp.clip(jnp.exp(math.log(1.0) - 2.3025851 * jax.random.uniform(streams_of[2], (TOKENS, TOPK), jnp.float32) ** block_levels(streams_of[2], (TOKENS, TOPK), ((0, 32),), -0.2, 0.2)), 0.1, 1.0)
    token_tenant_index = touch_ends(jax.random.randint(streams_of[3], (TOKENS,), 0, TENANT_TOTAL), jax.random.fold_in(streams_of[3], 1), 0, TENANT_TOTAL - 1).astype(jnp.int32)
    adapted = touch_ends((jax.random.randint(streams_of[4], (TENANT_TOTAL, EXPERT_TOTAL), 0, 4) < 3).astype(jnp.int32), jax.random.fold_in(streams_of[4], 1), 0, 1)
    gate_up_weight = bell_draw(streams_of[5], (EXPERT_TOTAL, MODEL_DIMENSION, 2 * EXPERT_HIDDEN), MODEL_DIMENSION ** -0.5, 0.125, ((0, 16), (1, 2)))
    down_weight = bell_draw(streams_of[6], (EXPERT_TOTAL, EXPERT_HIDDEN, MODEL_DIMENSION), EXPERT_HIDDEN ** -0.5, 0.3125, ((0, 16), (2, 2)))
    adapter_input_factors = bell_draw(streams_of[7], (TENANT_TOTAL, EXPERT_TOTAL, 2 * ADAPTER_RANK, MODEL_DIMENSION), MODEL_DIMENSION ** -0.5, 0.125, ((0, 2), (1, 16)))
    adapter_output_factors = bell_draw(streams_of[8], (TENANT_TOTAL, EXPERT_TOTAL, 2 * ADAPTER_RANK, EXPERT_HIDDEN), 0.15, 0.8984375, ((0, 2), (1, 16)))
    return dict(tokens=tokens, chosen_expert_index=chosen_expert_index, router_weight_logits=router_weight_logits, token_tenant_index=token_tenant_index, adapted=adapted, gate_up_weight=gate_up_weight, down_weight=down_weight, adapter_input_factors=adapter_input_factors, adapter_output_factors=adapter_output_factors)


def widen_factors(factor_up):
    rank_half = factor_up.shape[1] // 2
    hidden = factor_up.shape[2]
    zeros_part = jnp.zeros((factor_up.shape[0], rank_half, hidden), factor_up.dtype)
    upper = jnp.concatenate([factor_up[:, :rank_half], zeros_part], axis=2)
    lower = jnp.concatenate([zeros_part, factor_up[:, rank_half:]], axis=2)
    return jnp.concatenate([upper, lower], axis=1).reshape(-1, 2 * hidden)


def adapter_term(flat_rows, tenant_codes, factor_in, factor_up, adapted_col):
    tenants = factor_in.shape[0]
    rank_full = factor_in.shape[1]
    model_width = factor_in.shape[2]
    low_rank = lax.dot_general(flat_rows, factor_in.reshape(-1, model_width), (((1,), (1,)), ((), ())), preferred_element_type=jnp.float32)
    chooser = ((tenant_codes[:, None] == jnp.arange(tenants, dtype=jnp.int32)[None, :]) * adapted_col[None, :]).astype(jnp.float32)
    low_rank = (low_rank.reshape(-1, tenants, rank_full) * chooser[:, :, None]).reshape(flat_rows.shape[0], -1).astype(jnp.bfloat16)
    return jnp.dot(low_rank, widen_factors(factor_up), preferred_element_type=jnp.float32)


def reference(tokens, chosen_expert_index, router_weight_logits, token_tenant_index, adapted, gate_up_weight, down_weight, adapter_input_factors, adapter_output_factors):
    tok_total, model_width = tokens.shape
    experts = gate_up_weight.shape[0]
    hidden = down_weight.shape[1]
    blocks = tok_total // TOK_DEV
    per_block = TOK_DEV * TOPK
    block_ids = chosen_expert_index.reshape(blocks, per_block)
    onehot = (block_ids[:, :, None] == jnp.arange(experts, dtype=jnp.int32)[None, None, :]).astype(jnp.int32)
    position = jnp.sum((jnp.cumsum(onehot, axis=1) - 1) * onehot, axis=2)
    slot_index = block_ids * (blocks * CAP) + jnp.arange(blocks, dtype=jnp.int32)[:, None] * CAP + position
    route_rows = tok_total * TOPK
    position_row = jnp.full((experts * blocks * CAP,), route_rows, jnp.int32)
    position_row = position_row.at[slot_index.reshape(-1)].set(jnp.arange(route_rows, dtype=jnp.int32)).reshape(experts, blocks * CAP)
    shares = router_weight_logits / jnp.sum(router_weight_logits, axis=1, keepdims=True)
    share_flat = jnp.concatenate([shares.reshape(-1), jnp.zeros((1,), jnp.float32)])
    padded = jnp.concatenate([tokens, jnp.zeros((1, model_width), tokens.dtype)])
    tenant_pad = jnp.concatenate([token_tenant_index, jnp.full((1,), -1, jnp.int32)])

    def expert_step(accum, inputs):
        row_index, weight_in, weight_out, factor_in, factor_up, adapted_col = inputs
        token_index = row_index // TOPK
        flat_rows = padded[token_index]
        pre_act = jnp.dot(flat_rows, weight_in, preferred_element_type=jnp.float32)
        pre_act = pre_act + adapter_term(flat_rows, tenant_pad[token_index], factor_in, factor_up, adapted_col)
        activation = (jax.nn.silu(pre_act[:, :hidden]) * pre_act[:, hidden:]).astype(jnp.bfloat16)
        expert_out = jnp.dot(activation, weight_out, preferred_element_type=jnp.float32).astype(jnp.bfloat16)
        contribution = expert_out.astype(jnp.float32) * share_flat[row_index][:, None]
        return accum.at[token_index].add(contribution), None

    accum = jnp.zeros((tok_total + 1, model_width), jnp.float32)
    stacked_rows = (position_row, gate_up_weight, down_weight, jnp.swapaxes(adapter_input_factors, 0, 1), jnp.swapaxes(adapter_output_factors, 0, 1), jnp.swapaxes(adapted, 0, 1))
    accum, unused = lax.scan(expert_step, accum, stacked_rows)
    return accum[:tok_total].astype(jnp.bfloat16)
```

```python
import functools

import jax
import jax.numpy as jnp
from jax import lax
from jax.experimental import pallas as pl
from jax.experimental.pallas import tpu as pltpu
from jax.sharding import Mesh, PartitionSpec as P


F32 = jnp.float32
BF16 = jnp.bfloat16
LANES = 128
INNER = 4
VMEM = pl.BlockSpec(memory_space=pltpu.VMEM)
SMEM = pl.BlockSpec(memory_space=pltpu.SMEM)


def call(body, outs, ins, flops, cost_bytes, name):
    smem = ins[0]
    return pl.pallas_call(
        body,
        out_shape=outs,
        in_specs=[SMEM] * len(smem) + [VMEM] * (len(ins) - 1),
        out_specs=jax.tree.map(lambda _: VMEM, outs),
        compiler_params=pltpu.CompilerParams(vmem_limit_bytes=20 * 1024 * 1024),
        cost_estimate=pl.CostEstimate(flops=flops, bytes_accessed=cost_bytes, transcendentals=0),
        name=name,
    )(*smem, *ins[1:])


def iota(shape, dim):
    return lax.broadcasted_iota(jnp.int32, shape, dim)


def packing(meta, expert, top, rows):
    tok = meta.shape[0]
    lane = iota(meta.shape, 1)
    chosen = jnp.where(lane < top, meta, -1.0)
    named = jnp.zeros(meta.shape, F32)
    hits = []
    for q in range(INNER):
        target = lax.bitwise_xor(expert, q).astype(F32)
        hit = jnp.max(jnp.where(chosen == target, 1.0, 0.0), axis=1, keepdims=True)
        hits.append(hit)
        named = jnp.where(lane == q, hit, named)
    below = jnp.where(iota((tok, tok), 1) < iota((tok, tok), 0), 1.0, 0.0).astype(BF16)
    place = jnp.dot(below, named.astype(BF16), preferred_element_type=F32)
    slots = []
    for q in range(INNER):
        slot = jnp.where(hits[q] > 0.0, place[:, q : q + 1], -1.0)
        slots.append(slot)
    return slots


def one_hot(slots, rows):
    tok = slots[0].shape[0]
    lane = iota((tok, INNER * rows), 1).astype(F32)
    picked = jnp.zeros((tok, INNER * rows), F32)
    for q in range(INNER):
        at = jnp.where(slots[q] >= 0.0, slots[q] + float(q * rows), -1.0)
        picked = jnp.where(lane == at, 1.0, picked)
    return picked.astype(BF16)


def pack_rows(expert, meta, wide, outs, top, rows):
    picked = one_hot(packing(meta, expert, top, rows), rows)
    got = lax.dot_general(picked, wide, (((0,), (0,)), ((), ())), preferred_element_type=F32).astype(BF16)
    for q in range(INNER):
        outs[q][...] = got[q * rows : (q + 1) * rows]


def first_body(top, rows, expert_ref, tok_ref, ids_ref, tenant_ref, logit_ref, ext_ref, *outs):
    tok, width = tok_ref.shape
    share = logit_ref[...] / jnp.sum(logit_ref[...], axis=0, keepdims=True)
    high = share.astype(BF16).astype(F32)
    mid = (share - high).astype(BF16).astype(F32)
    low = share - high - mid
    pad = jnp.zeros((32 - top, tok), F32)
    meta_t = jnp.concatenate(
        [
            ids_ref[...].astype(F32),
            jnp.broadcast_to(tenant_ref[...].astype(F32), (8, tok)),
            jnp.zeros((32 - top - 8, tok), F32),
            high,
            pad,
            mid,
            pad,
            low,
            pad,
        ],
        axis=0,
    )
    meta = meta_t.T
    ext_ref[:, :width] = tok_ref[...]
    ext_ref[:, width:] = meta.astype(BF16)
    pack_rows(expert_ref[0], meta, ext_ref[...], outs, top, rows)


def pack_body(top, rows, width, expert_ref, ext_ref, *outs):
    meta = ext_ref[:, width:].astype(F32)
    pack_rows(expert_ref[0], meta, ext_ref[...], outs, top, rows)


def expert_body(top, rows, stores, scal_ref, adapted_ref, *refs):
    xs, refs = refs[:INNER], refs[INNER:]
    ups, refs = refs[:stores], refs[stores:]
    downs, refs = refs[:stores], refs[stores:]
    fin_ref, fup_ref = refs[0], refs[1]
    outs, x_ref = refs[2 : 2 + INNER], refs[2 + INNER]
    store = scal_ref[1]
    width = ups[0].shape[0] * stores
    hidden = downs[0].shape[0]
    for q in range(INNER):
        x_ref[q * rows : (q + 1) * rows] = xs[q][...]
    count = INNER * rows
    k = ups[0].shape[0]
    pre = None
    for r in range(stores):
        at = pl.multiple_of(lax.bitwise_xor(store, r) * k, LANES)
        part = jnp.dot(x_ref[:, pl.ds(at, k)], ups[r][...], preferred_element_type=F32)
        pre = part if pre is None else pre + part
    low = lax.dot_general(
        x_ref[:, :width], fin_ref[...], (((1,), (1,)), ((), ())), preferred_element_type=F32
    )
    ranks = low.shape[1]
    tenants = adapted_ref.shape[0]
    rank = ranks // tenants
    held = tenants // stores
    lane = iota((1, ranks), 1)
    shard = lax.bitwise_xor(lane // (rank * held), store)
    tenant = shard * held + (lane // rank) % held
    allowed = jnp.zeros((1, ranks), F32)
    for u in range(tenants):
        allowed = jnp.where(tenant == u, adapted_ref[u].astype(F32), allowed)
    code = x_ref[:, width + top : width + top + 1].astype(F32)
    chooser = jnp.where(code == tenant.astype(F32), allowed, 0.0)
    low = (low * chooser).astype(BF16)
    half = (lane % rank) < rank // 2
    zero = jnp.zeros_like(low)
    gate = pre[:, :hidden] + jnp.dot(jnp.where(half, low, zero), fup_ref[...], preferred_element_type=F32)
    up = pre[:, hidden:] + jnp.dot(jnp.where(half, zero, low), fup_ref[...], preferred_element_type=F32)
    act = (gate / (1.0 + jnp.exp(-gate)) * up).astype(BF16)
    n = downs[0].shape[1]
    for r in range(stores):
        at = pl.multiple_of(lax.bitwise_xor(store, r) * n, LANES)
        got = jnp.dot(act, downs[r][...], preferred_element_type=F32).astype(BF16)
        for q in range(INNER):
            outs[q][:, pl.ds(at, n)] = got[q * rows : (q + 1) * rows]


def weighted(expert, meta, ys, top, rows):
    slots = packing(meta, expert, top, rows)
    lane = iota(meta.shape, 1)
    chosen = jnp.where(lane < top, meta, -1.0)
    share = sum(pltpu.roll(meta, LANES - 32 * (i + 1), 1) for i in range(3))
    total = None
    for q in range(INNER):
        target = lax.bitwise_xor(expert, q).astype(F32)
        mine = jnp.sum(jnp.where(chosen == target, share, 0.0), axis=1, keepdims=True)
        spot = iota((meta.shape[0], rows), 1).astype(F32)
        spread = jnp.where(spot == slots[q], 1.0, 0.0).astype(BF16)
        part = jnp.dot(spread, ys[q][...], preferred_element_type=F32) * mine
        total = part if total is None else total + part
    return total


def partial_body(top, rows, width, expert_ref, ext_ref, *refs):
    meta = ext_ref[:, width:].astype(F32)
    refs[INNER][...] = weighted(expert_ref[0], meta, refs[:INNER], top, rows).astype(BF16)


def final_body(top, rows, width, expert_ref, ext_ref, *refs):
    meta = ext_ref[:, width:].astype(F32)
    total = weighted(expert_ref[0], meta, refs[:INNER], top, rows)
    for other in refs[INNER:-1]:
        total = total + other[...].astype(F32)
    refs[-1][...] = total.astype(BF16)


def swap(array, axis, distance):
    return lax.ppermute(array, axis, [(i, i ^ distance) for i in range(lax.axis_size(axis))])


def shards(
    tokens,
    chosen_expert_index,
    router_weight_logits,
    token_tenant_index,
    adapted,
    gate_up_weight,
    down_weight,
    adapter_input_factors,
    adapter_output_factors,
):
    tok, width = tokens.shape
    top = chosen_expert_index.shape[1]
    outer, stores = lax.axis_size("outer"), lax.axis_size("store")
    owners = outer * INNER
    cap = max(2, tok * top * 9 // (8 * owners))
    rows = -(-cap // 8) * 8
    hidden = down_weight.shape[1]
    wide = width + LANES
    expert = lax.axis_index("outer") * INNER + lax.axis_index("inner")
    store = lax.axis_index("store")
    scal = jnp.stack([expert, store]).astype(jnp.int32)
    packed = jax.ShapeDtypeStruct((rows, wide), BF16)
    returned = jax.ShapeDtypeStruct((rows, width), BF16)
    ext_shape = jax.ShapeDtypeStruct((tok, wide), BF16)
    sums = jax.ShapeDtypeStruct((tok, width), BF16)

    move_flops = 2 * tok * INNER * rows * width
    move_bytes = 2 * (tok + INNER * rows) * wide
    first = call(
        functools.partial(first_body, top, rows),
        [ext_shape] + [packed] * INNER,
        [[scal], tokens, chosen_expert_index.T, token_tenant_index.reshape(1, -1), router_weight_logits.T],
        move_flops,
        move_bytes,
        "first",
    )
    blocks = [first[0]]
    rows_of = [first[1:]]
    for d in range(1, outer):
        blocks.append(swap(first[0], "outer", d))

    ups = [gate_up_weight[0]]
    downs = [down_weight[0]]
    fin = [adapter_input_factors.reshape(-1, width)]
    fup = [adapter_output_factors.reshape(-1, hidden)]
    for r in range(1, stores):
        ups.append(swap(ups[0], "store", r))
        downs.append(swap(downs[0], "store", r))
        fin.append(swap(fin[0], "store", r))
        fup.append(swap(fup[0], "store", r))
    fin = jnp.concatenate(fin, axis=0)
    fup = jnp.concatenate(fup, axis=0)

    for d in range(1, outer):
        rows_of.append(
            call(
                functools.partial(pack_body, top, rows, width),
                [packed] * INNER,
                [[scal], blocks[d]],
                move_flops,
                move_bytes,
                "pack",
            )
        )
    arrived = [[r[0]] + [swap(r[q], "inner", q) for q in range(1, INNER)] for r in rows_of]

    backs = []
    for d in range(outer):
        got = pl.pallas_call(
            functools.partial(expert_body, top, rows, stores),
            out_shape=[returned] * INNER,
            in_specs=[SMEM] * 2 + [VMEM] * (INNER + 2 * stores + 2),
            out_specs=[VMEM] * INNER,
            scratch_shapes=[pltpu.VMEM((INNER * rows, wide), BF16)],
            compiler_params=pltpu.CompilerParams(vmem_limit_bytes=28 * 1024 * 1024),
            cost_estimate=pl.CostEstimate(
                flops=2 * INNER * rows * width * hidden * 3, bytes_accessed=6 * width * hidden, transcendentals=0
            ),
            name="expert",
        )(scal, adapted[:, 0], *arrived[d], *ups, *downs, fin, fup)
        backs.append([got[0]] + [swap(got[q], "inner", q) for q in range(1, INNER)])

    others = []
    for d in range(1, outer):
        part = call(
            functools.partial(partial_body, top, rows, width),
            sums,
            [[scal], blocks[d]] + backs[d],
            move_flops,
            move_bytes,
            "partial",
        )
        others.append(swap(part, "outer", d))
    return call(
        functools.partial(final_body, top, rows, width),
        sums,
        [[scal], blocks[0]] + backs[0] + others,
        move_flops,
        move_bytes,
        "final",
    )


def solution(mesh):
    owners, stores = mesh.devices.shape
    grid = Mesh(mesh.devices.reshape(owners // INNER, INNER, stores), ("outer", "inner", "store"))
    expert, both = ("outer", "inner"), ("outer", "inner", "store")
    placed = (
        P(both, None),
        P(both, None),
        P(both, None),
        P(both),
        P(None, expert),
        P(expert, "store", None),
        P(expert, None, "store"),
        P("store", expert, None, None),
        P("store", expert, None, None),
    )
    return jax.shard_map(shards, mesh=grid, in_specs=placed, out_specs=P(both, None), check_vma=False)
```

```python
import functools

import jax
import jax.numpy as jnp
from jax import lax
from jax.experimental import pallas as pl
from jax.experimental.pallas import tpu as pltpu
from jax.sharding import Mesh, PartitionSpec as P


F32 = jnp.float32
BF16 = jnp.bfloat16
LANES = 128
INNER = 4
VMEM = pl.BlockSpec(memory_space=pltpu.VMEM)
SMEM = pl.BlockSpec(memory_space=pltpu.SMEM)


def call(body, outs, ins, flops, cost_bytes):
    smem = ins[0]
    return pl.pallas_call(
        body,
        out_shape=outs,
        in_specs=[SMEM] * len(smem) + [VMEM] * (len(ins) - 1),
        out_specs=jax.tree.map(lambda _: VMEM, outs),
        compiler_params=pltpu.CompilerParams(vmem_limit_bytes=20 * 1024 * 1024),
        cost_estimate=pl.CostEstimate(flops=flops, bytes_accessed=cost_bytes, transcendentals=0),
    )(*smem, *ins[1:])


def iota(shape, dim):
    return lax.broadcasted_iota(jnp.int32, shape, dim)


def packing(meta, expert, top):
    tok = meta.shape[0]
    lane = iota(meta.shape, 1)
    chosen = jnp.where(lane < top, meta, -1.0)
    named = jnp.zeros(meta.shape, F32)
    hits = []
    for q in range(INNER):
        target = lax.bitwise_xor(expert, q).astype(F32)
        hit = jnp.max(jnp.where(chosen == target, 1.0, 0.0), axis=1, keepdims=True)
        hits.append(hit)
        named = jnp.where(lane == q, hit, named)
    below = jnp.where(iota((tok, tok), 1) < iota((tok, tok), 0), 1.0, 0.0).astype(BF16)
    place = jnp.dot(below, named.astype(BF16), preferred_element_type=F32)
    slots = []
    for q in range(INNER):
        slot = jnp.where(hits[q] > 0.0, place[:, q : q + 1], -1.0)
        slots.append(slot)
    return slots


def one_hot(slots, rows):
    tok = slots[0].shape[0]
    lane = iota((tok, INNER * rows), 1).astype(F32)
    picked = jnp.zeros((tok, INNER * rows), F32)
    for q in range(INNER):
        at = jnp.where(slots[q] >= 0.0, slots[q] + float(q * rows), -1.0)
        picked = jnp.where(lane == at, 1.0, picked)
    return picked.astype(BF16)


def pack_rows(slots, wide, outs, rows):
    picked = one_hot(slots, rows)
    got = lax.dot_general(picked, wide, (((0,), (0,)), ((), ())), preferred_element_type=F32).astype(BF16)
    for q in range(INNER):
        outs[q][...] = got[q * rows : (q + 1) * rows]


def first_body(top, rows, expert_ref, tok_any, meta_ref, ext_ref, *refs):
    outs, sem = refs[:INNER], refs[INNER]
    tok, width = tok_any.shape
    copy = pltpu.make_async_copy(tok_any, ext_ref.at[:, pl.ds(0, width)], sem)
    copy.start()
    logits = meta_ref[top + 8 :]
    share = logits / jnp.sum(logits, axis=0, keepdims=True)
    high = share.astype(BF16).astype(F32)
    mid = (share - high).astype(BF16).astype(F32)
    low = share - high - mid
    pad = jnp.zeros((32 - top, tok), F32)
    meta_t = jnp.concatenate(
        [
            meta_ref[: top + 8],
            jnp.zeros((32 - top - 8, tok), F32),
            high,
            pad,
            mid,
            pad,
            low,
            pad,
        ],
        axis=0,
    )
    meta = meta_t.T
    ext_ref[:, width:] = meta.astype(BF16)
    slots = packing(meta, expert_ref[0], top)
    copy.wait()
    pack_rows(slots, ext_ref[...], outs, rows)


def either(scal_ref, pair, columns=slice(None)):
    return jnp.where(scal_ref[2] > 0, pair[1][:, columns], pair[0][:, columns])


def pack_body(top, rows, width, scal_ref, inner_ref, end_ref, *outs):
    wide = either(scal_ref, (inner_ref, end_ref))
    pack_rows(packing(wide[:, width:].astype(F32), scal_ref[0], top), wide, outs, rows)


def expert_body(top, rows, stores, parts, scal_ref, adapted_ref, *refs):
    xs, refs = refs[:INNER], refs[INNER:]
    ups, refs = refs[:stores], refs[stores:]
    downs, refs = refs[:stores], refs[stores:]
    fins, refs = refs[:stores], refs[stores:]
    fups, refs = refs[:stores], refs[stores:]
    outs, (x_ref, fin_ref, fup_ref, y_ref) = refs[: INNER * parts], refs[INNER * parts :]
    store = scal_ref[1]
    width = ups[0].shape[0] * stores
    hidden = downs[0].shape[0]
    for q in range(INNER):
        x_ref[q * rows : (q + 1) * rows] = xs[q][...]
    k = ups[0].shape[0]
    pre = None
    for r in range(stores):
        at = pl.multiple_of(lax.bitwise_xor(store, r) * k, LANES)
        part = jnp.dot(x_ref[:, pl.ds(at, k)], ups[r][...], preferred_element_type=F32)
        pre = part if pre is None else pre + part
    tenants = adapted_ref.shape[0]
    held = tenants // stores
    part = fins[0].shape[0]
    rank = part // held
    for r in range(stores):
        fin_ref[r * part : (r + 1) * part] = fins[r][...]
        fup_ref[r * part : (r + 1) * part] = fups[r][...]
    lane = iota((1, stores * part), 1)
    half = (lane % rank) < rank // 2
    tenant = lax.bitwise_xor(store, lane // part) * held + (lane // rank) % held
    allowed = jnp.zeros(lane.shape, F32)
    for u in range(tenants):
        allowed = jnp.where(tenant == u, adapted_ref[u].astype(F32), allowed)
    code = x_ref[:, width + top : width + top + 1].astype(F32)
    low = lax.dot_general(
        x_ref[:, :width], fin_ref[...], (((1,), (1,)), ((), ())), preferred_element_type=F32
    )
    low = (low * jnp.where(code == tenant.astype(F32), allowed, 0.0)).astype(BF16)
    zero = jnp.zeros_like(low)
    gate = pre[:, :hidden] + jnp.dot(jnp.where(half, low, zero), fup_ref[...], preferred_element_type=F32)
    up = pre[:, hidden:] + jnp.dot(jnp.where(half, zero, low), fup_ref[...], preferred_element_type=F32)
    act = (gate / (1.0 + jnp.exp(-gate)) * up).astype(BF16)
    n = downs[0].shape[1]
    for r in range(stores):
        at = pl.multiple_of(lax.bitwise_xor(store, r) * n, LANES)
        y_ref[:, pl.ds(at, n)] = jnp.dot(act, downs[r][...], preferred_element_type=F32).astype(BF16)
    each = width // parts
    for q in range(INNER):
        for i in range(parts):
            outs[q * parts + i][...] = y_ref[q * rows : (q + 1) * rows, i * each : (i + 1) * each]


def weighted(expert, meta, ys, top, rows):
    slots = packing(meta, expert, top)
    lane = iota(meta.shape, 1)
    chosen = jnp.where(lane < top, meta, -1.0)
    share = sum(pltpu.roll(meta, LANES - 32 * (i + 1), 1) for i in range(3))
    total = None
    for q in range(INNER):
        target = lax.bitwise_xor(expert, q).astype(F32)
        mine = jnp.sum(jnp.where(chosen == target, share, 0.0), axis=1, keepdims=True)
        spot = iota((meta.shape[0], rows), 1).astype(F32)
        spread = jnp.where(spot == slots[q], 1.0, 0.0).astype(BF16)
        part = jnp.dot(spread, ys[q][...], preferred_element_type=F32) * mine
        total = part if total is None else total + part
    return total


def partial_body(top, rows, width, scal_ref, inner_ref, end_ref, *refs):
    meta = either(scal_ref, (inner_ref, end_ref), slice(width, None)).astype(F32)
    refs[INNER][...] = weighted(scal_ref[0], meta, refs[:INNER], top, rows).astype(BF16)


def final_body(top, rows, width, splits, expert_ref, ext_ref, *refs):
    meta = ext_ref[:, width:].astype(F32)
    total = weighted(expert_ref[0], meta, refs[:INNER], top, rows)
    others, out = list(refs[INNER:-1]), refs[-1]
    for count in splits:
        pieces = [others.pop(0)[...].astype(F32) for _ in range(count)]
        total = total + (pieces[0] if count == 1 else jnp.concatenate(pieces, axis=1))
    out[...] = total.astype(BF16)


def swap(array, axis, distance):
    return lax.ppermute(array, axis, [(i, i ^ distance) for i in range(lax.axis_size(axis))])


def spread(block, outer):
    if outer != 4:
        return [(block, block)] + [(got, got) for got in (swap(block, "outer", d) for d in range(1, outer))]
    middle, outward = [(1, 2), (2, 1)], [(1, 0), (2, 3)]
    near = swap(block, "outer", 1)
    over = lax.ppermute(block, "outer", middle)
    over_near = lax.ppermute(near, "outer", middle)
    end_over = lax.ppermute(over, "outer", outward)
    end_over_near = lax.ppermute(over_near, "outer", outward)
    return [(block, block), (near, near), (over, end_over), (over_near, end_over_near)]


def column_parts(d, outer):
    return 2 if outer == 4 and d in (2, 3) else 1


def shards(
    tokens,
    chosen_expert_index,
    router_weight_logits,
    token_tenant_index,
    adapted,
    gate_up_weight,
    down_weight,
    adapter_input_factors,
    adapter_output_factors,
):
    tok, width = tokens.shape
    top = chosen_expert_index.shape[1]
    outer, stores = lax.axis_size("outer"), lax.axis_size("store")
    owners = outer * INNER
    cap = max(2, tok * top * 9 // (8 * owners))
    rows = -(-cap // 8) * 8
    hidden = down_weight.shape[1]
    wide = width + LANES
    expert = lax.axis_index("outer") * INNER + lax.axis_index("inner")
    store = lax.axis_index("store")
    place = lax.axis_index("outer")
    ends = jnp.logical_or(place == 0, place == outer - 1)
    scal = jnp.stack([expert, store, ends.astype(jnp.int32)]).astype(jnp.int32)
    packed = jax.ShapeDtypeStruct((rows, wide), BF16)
    ext_shape = jax.ShapeDtypeStruct((tok, wide), BF16)
    sums = jax.ShapeDtypeStruct((tok, width), BF16)

    move_flops = 2 * tok * INNER * rows * width
    move_bytes = 2 * (tok + INNER * rows) * wide
    meta = jnp.concatenate(
        [
            chosen_expert_index.T.astype(F32),
            jnp.broadcast_to(token_tenant_index.astype(F32), (8, tok)),
            router_weight_logits.T,
        ]
    )
    first = pl.pallas_call(
        functools.partial(first_body, top, rows),
        out_shape=[ext_shape] + [packed] * INNER,
        in_specs=[SMEM, pl.BlockSpec(memory_space=pl.ANY), VMEM],
        out_specs=[VMEM] * (1 + INNER),
        scratch_shapes=[pltpu.SemaphoreType.DMA],
        compiler_params=pltpu.CompilerParams(vmem_limit_bytes=20 * 1024 * 1024),
        cost_estimate=pl.CostEstimate(flops=move_flops, bytes_accessed=move_bytes, transcendentals=0),
        name="first",
    )(scal, tokens, meta)
    blocks = spread(first[0], outer)
    rows_of = [first[1:]]

    ups = [gate_up_weight[0]]
    downs = [down_weight[0]]
    fin = [adapter_input_factors.reshape(-1, width)]
    fup = [adapter_output_factors.reshape(-1, hidden)]
    for r in range(1, stores):
        ups.append(swap(ups[0], "store", r))
        downs.append(swap(downs[0], "store", r))
        fin.append(swap(fin[0], "store", r))
        fup.append(swap(fup[0], "store", r))

    for d in range(1, outer):
        rows_of.append(
            call(
                functools.partial(pack_body, top, rows, width),
                [packed] * INNER,
                [[scal], *blocks[d]],
                move_flops,
                move_bytes,
            )
        )
    arrived = [[r[0]] + [swap(r[q], "inner", q) for q in range(1, INNER)] for r in rows_of]

    backs = []
    for d in range(outer):
        parts = column_parts(d, outer)
        kernel = pl.pallas_call(
            functools.partial(expert_body, top, rows, stores, parts),
            out_shape=[jax.ShapeDtypeStruct((rows, width // parts), BF16)] * (INNER * parts),
            in_specs=[SMEM] * 2 + [VMEM] * (INNER + 4 * stores),
            out_specs=[VMEM] * (INNER * parts),
            scratch_shapes=[
                pltpu.VMEM((INNER * rows, wide), BF16),
                pltpu.VMEM((stores * fin[0].shape[0], width), BF16),
                pltpu.VMEM((stores * fin[0].shape[0], hidden), BF16),
                pltpu.VMEM((INNER * rows, width), BF16),
            ],
            compiler_params=pltpu.CompilerParams(vmem_limit_bytes=28 * 1024 * 1024),
            cost_estimate=pl.CostEstimate(
                flops=2 * INNER * rows * width * hidden * 3, bytes_accessed=6 * width * hidden, transcendentals=0
            ),
            name="expert",
        )
        got = kernel(scal, adapted[:, 0], *arrived[d], *ups, *downs, *fin, *fup)
        backs.append([[got[i]] + [swap(got[q * parts + i], "inner", q) for q in range(1, INNER)] for i in range(parts)])

    def partial(d, i=0):
        return call(
            functools.partial(partial_body, top, rows, width),
            jax.ShapeDtypeStruct((tok, width // len(backs[d])), BF16),
            [[scal], *blocks[d], *backs[d][i]],
            move_flops,
            move_bytes,
        )

    if outer == 4:
        others = []
        for d, targets in ((2, [(1, 2), (2, 1)]), (3, [(1, 3), (2, 0)])):
            others.append([])
            for i in range(len(backs[d])):
                part = partial(d, i)
                more = lax.ppermute(part, "outer", [(0, 1), (3, 2)])
                part = (part.astype(F32) + more.astype(F32)).astype(BF16)
                others[-1].append(lax.ppermute(part, "outer", targets))
        others.append([swap(partial(1), "outer", 1)])
    else:
        others = [[swap(partial(d), "outer", d)] for d in range(1, outer)]
    return call(
        functools.partial(final_body, top, rows, width, [len(other) for other in others]),
        sums,
        [[scal], first[0]] + backs[0][0] + sum(others, []),
        move_flops,
        move_bytes,
    )


def solution(mesh):
    owners, stores = mesh.devices.shape
    grid = Mesh(mesh.devices.reshape(owners // INNER, INNER, stores), ("outer", "inner", "store"))
    expert, both = ("outer", "inner"), ("outer", "inner", "store")
    placed = (
        P(both, None),
        P(both, None),
        P(both, None),
        P(both),
        P(None, expert),
        P(expert, "store", None),
        P(expert, None, "store"),
        P("store", expert, None, None),
        P("store", expert, None, None),
    )

    return jax.shard_map(shards, mesh=grid, in_specs=placed, out_specs=P(both, None), check_vma=False)
```

```python
import functools

import jax
import jax.numpy as jnp
from jax import lax
from jax.experimental import pallas as pl
from jax.experimental.pallas import tpu as pltpu
from jax.sharding import Mesh, PartitionSpec as P


F32 = jnp.float32
BF16 = jnp.bfloat16
LANES = 128
INNER = 4
VMEM = pl.BlockSpec(memory_space=pltpu.VMEM)
SMEM = pl.BlockSpec(memory_space=pltpu.SMEM)


def call(body, outs, ins, flops, cost_bytes):
    smem = ins[0]
    return pl.pallas_call(
        body,
        out_shape=outs,
        in_specs=[SMEM] * len(smem) + [VMEM] * (len(ins) - 1),
        out_specs=jax.tree.map(lambda _: VMEM, outs),
        compiler_params=pltpu.CompilerParams(vmem_limit_bytes=20 * 1024 * 1024),
        cost_estimate=pl.CostEstimate(flops=flops, bytes_accessed=cost_bytes, transcendentals=0),
    )(*smem, *ins[1:])


def iota(shape, dim):
    return lax.broadcasted_iota(jnp.int32, shape, dim)


def packing(meta, expert, top):
    tok = meta.shape[0]
    lane = iota(meta.shape, 1)
    chosen = jnp.where(lane < top, meta, -1.0)
    named = jnp.zeros(meta.shape, F32)
    hits = []
    for q in range(INNER):
        target = lax.bitwise_xor(expert, q).astype(F32)
        hit = jnp.max(jnp.where(chosen == target, 1.0, 0.0), axis=1, keepdims=True)
        hits.append(hit)
        named = jnp.where(lane == q, hit, named)
    below = jnp.where(iota((tok, tok), 1) < iota((tok, tok), 0), 1.0, 0.0).astype(BF16)
    place = jnp.dot(below, named.astype(BF16), preferred_element_type=F32)
    slots = []
    for q in range(INNER):
        slot = jnp.where(hits[q] > 0.0, place[:, q : q + 1], -1.0)
        slots.append(slot)
    return slots


def one_hot(slots, rows):
    tok = slots[0].shape[0]
    lane = iota((tok, INNER * rows), 1).astype(F32)
    picked = jnp.zeros((tok, INNER * rows), F32)
    for q in range(INNER):
        at = jnp.where(slots[q] >= 0.0, slots[q] + float(q * rows), -1.0)
        picked = jnp.where(lane == at, 1.0, picked)
    return picked.astype(BF16)


def pack_rows(slots, wide, outs, rows):
    picked = one_hot(slots, rows)
    got = lax.dot_general(picked, wide, (((0,), (0,)), ((), ())), preferred_element_type=F32).astype(BF16)
    for q in range(INNER):
        outs[q][...] = got[q * rows : (q + 1) * rows]


def first_body(top, rows, expert_ref, tok_any, meta_ref, ext_ref, *refs):
    outs, sem = refs[:INNER], refs[INNER]
    tok, width = tok_any.shape
    copy = pltpu.make_async_copy(tok_any, ext_ref.at[:, pl.ds(0, width)], sem)
    copy.start()
    logits = meta_ref[top + 8 :]
    share = logits / jnp.sum(logits, axis=0, keepdims=True)
    high = share.astype(BF16).astype(F32)
    mid = (share - high).astype(BF16).astype(F32)
    low = share - high - mid
    pad = jnp.zeros((32 - top, tok), F32)
    meta_t = jnp.concatenate(
        [
            meta_ref[: top + 8],
            jnp.zeros((32 - top - 8, tok), F32),
            high,
            pad,
            mid,
            pad,
            low,
            pad,
        ],
        axis=0,
    )
    meta = meta_t.T
    ext_ref[:, width:] = meta.astype(BF16)
    slots = packing(meta, expert_ref[0], top)
    copy.wait()
    pack_rows(slots, ext_ref[...], outs, rows)


def pack_body(top, rows, width, scal_ref, *refs):
    wide = either(scal_ref, refs[:-INNER])
    pack_rows(packing(wide[:, width:].astype(F32), scal_ref[0], top), wide, refs[-INNER:], rows)


def expert_body(top, rows, stores, parts, scal_ref, adapted_ref, *refs):
    xs, refs = refs[:INNER], refs[INNER:]
    ups, refs = refs[:stores], refs[stores:]
    downs, refs = refs[:stores], refs[stores:]
    fins, refs = refs[:stores], refs[stores:]
    fups, refs = refs[:stores], refs[stores:]
    outs, (x_ref, fin_ref, fup_ref, y_ref) = refs[: INNER * parts], refs[INNER * parts :]
    store = scal_ref[1]
    width = ups[0].shape[0] * stores
    hidden = downs[0].shape[0]
    for q in range(INNER):
        x_ref[q * rows : (q + 1) * rows] = xs[q][...]
    k = ups[0].shape[0]
    pre = None
    for r in range(stores):
        at = pl.multiple_of(lax.bitwise_xor(store, r) * k, LANES)
        part = jnp.dot(x_ref[:, pl.ds(at, k)], ups[r][...], preferred_element_type=F32)
        pre = part if pre is None else pre + part
    tenants = adapted_ref.shape[0]
    held = tenants // stores
    part = fins[0].shape[0]
    rank = part // held
    for r in range(stores):
        fin_ref[r * part : (r + 1) * part] = fins[r][...]
        fup_ref[r * part : (r + 1) * part] = fups[r][...]
    lane = iota((1, stores * part), 1)
    half = (lane % rank) < rank // 2
    tenant = lax.bitwise_xor(store, lane // part) * held + (lane // rank) % held
    allowed = jnp.zeros(lane.shape, F32)
    for u in range(tenants):
        allowed = jnp.where(tenant == u, adapted_ref[u].astype(F32), allowed)
    code = x_ref[:, width + top : width + top + 1].astype(F32)
    low = lax.dot_general(
        x_ref[:, :width], fin_ref[...], (((1,), (1,)), ((), ())), preferred_element_type=F32
    )
    low = (low * jnp.where(code == tenant.astype(F32), allowed, 0.0)).astype(BF16)
    zero = jnp.zeros_like(low)
    gate = pre[:, :hidden] + jnp.dot(jnp.where(half, low, zero), fup_ref[...], preferred_element_type=F32)
    up = pre[:, hidden:] + jnp.dot(jnp.where(half, zero, low), fup_ref[...], preferred_element_type=F32)
    act = (gate / (1.0 + jnp.exp(-gate)) * up).astype(BF16)
    n = downs[0].shape[1]
    for r in range(stores):
        at = pl.multiple_of(lax.bitwise_xor(store, r) * n, LANES)
        y_ref[:, pl.ds(at, n)] = jnp.dot(act, downs[r][...], preferred_element_type=F32).astype(BF16)
    each = width // parts
    for q in range(INNER):
        for i in range(parts):
            outs[q * parts + i][...] = y_ref[q * rows : (q + 1) * rows, i * each : (i + 1) * each]


def weighted(expert, meta, ys, top, rows):
    slots = packing(meta, expert, top)
    lane = iota(meta.shape, 1)
    chosen = jnp.where(lane < top, meta, -1.0)
    share = sum(pltpu.roll(meta, LANES - 32 * (i + 1), 1) for i in range(3))
    total = None
    for q in range(INNER):
        target = lax.bitwise_xor(expert, q).astype(F32)
        mine = jnp.sum(jnp.where(chosen == target, share, 0.0), axis=1, keepdims=True)
        spot = iota((meta.shape[0], rows), 1).astype(F32)
        spread = jnp.where(spot == slots[q], 1.0, 0.0).astype(BF16)
        part = jnp.dot(spread, ys[q][...], preferred_element_type=F32) * mine
        total = part if total is None else total + part
    return total


def partial_body(top, rows, width, held, scal_ref, *refs):
    meta = either(scal_ref, refs[:held], slice(width, None)).astype(F32)
    refs = refs[held:]
    total = weighted(scal_ref[0], meta, refs[:INNER], top, rows)
    for other in refs[INNER:-1]:
        total = total + other[...].astype(F32)
    refs[-1][...] = total.astype(BF16)


def final_body(top, rows, width, splits, scal_ref, ext_ref, *refs):
    total = weighted(scal_ref[0], ext_ref[:, width:].astype(F32), refs[:INNER], top, rows)
    others, out = list(refs[INNER:-1]), refs[-1]
    for count in splits:
        pieces = [others.pop(0)[...].astype(F32) for _ in range(count)]
        total = total + (pieces[0] if count == 1 else jnp.concatenate(pieces, axis=1))
    out[...] = total.astype(BF16)


def swap(array, axis, distance):
    return lax.ppermute(array, axis, [(i, i ^ distance) for i in range(lax.axis_size(axis))])


def relayed(block):
    def send(array, pairs):
        return lax.ppermute(array, "outer", pairs)

    middle, outward = [(1, 2), (2, 1)], [(1, 0), (2, 3)]
    near = swap(block, "outer", 1)
    over = send(block, middle)
    over_near = send(near, middle)
    end_over = send(over, outward)
    end_over_near = send(over_near, outward)
    return [(block,), (near,), (over_near, end_over), (over, end_over_near)]


def either(scal_ref, block_refs, columns=slice(None)):
    if len(block_refs) == 1:
        return block_refs[0][:, columns]
    return jnp.where(scal_ref[2] > 0, block_refs[1][:, columns], block_refs[0][:, columns])


def lowest(d):
    return d & -d


def column_parts(d, outer):
    return 2 if outer == 4 and d in (2, 3) else 1


def shards(
    tokens,
    chosen_expert_index,
    router_weight_logits,
    token_tenant_index,
    adapted,
    gate_up_weight,
    down_weight,
    adapter_input_factors,
    adapter_output_factors,
):
    tok, width = tokens.shape
    top = chosen_expert_index.shape[1]
    outer, stores = lax.axis_size("outer"), lax.axis_size("store")
    owners = outer * INNER
    cap = max(2, tok * top * 9 // (8 * owners))
    rows = -(-cap // 8) * 8
    hidden = down_weight.shape[1]
    wide = width + LANES
    expert = lax.axis_index("outer") * INNER + lax.axis_index("inner")
    store = lax.axis_index("store")
    place = lax.axis_index("outer")
    ends = jnp.logical_or(place == 0, place == outer - 1)
    scal = jnp.stack([expert, store, ends.astype(jnp.int32)]).astype(jnp.int32)
    packed = jax.ShapeDtypeStruct((rows, wide), BF16)
    ext_shape = jax.ShapeDtypeStruct((tok, wide), BF16)
    sums = jax.ShapeDtypeStruct((tok, width), BF16)

    move_flops = 2 * tok * INNER * rows * width
    move_bytes = 2 * (tok + INNER * rows) * wide
    ints = jnp.pad(chosen_expert_index.T, ((0, top + 8), (0, 0)))
    ints = ints + jnp.pad(token_tenant_index.reshape(1, -1), ((top, top + 7), (0, 0)))
    meta = ints.astype(F32) + jnp.pad(router_weight_logits.T, ((top + 8, 0), (0, 0)))
    first = pl.pallas_call(
        functools.partial(first_body, top, rows),
        out_shape=[ext_shape] + [packed] * INNER,
        in_specs=[SMEM, pl.BlockSpec(memory_space=pl.ANY), VMEM],
        out_specs=[VMEM] * (1 + INNER),
        scratch_shapes=[pltpu.SemaphoreType.DMA],
        compiler_params=pltpu.CompilerParams(vmem_limit_bytes=20 * 1024 * 1024),
        cost_estimate=pl.CostEstimate(flops=move_flops, bytes_accessed=move_bytes, transcendentals=0),
        name="first",
    )(scal, tokens, meta)
    if outer == 4:
        blocks = relayed(first[0])
    else:
        blocks = [(first[0],)]
        for d in range(1, outer):
            blocks.append((swap(blocks[d - lowest(d)][0], "outer", lowest(d)),))
    rows_of = [first[1:]]

    ups = [gate_up_weight[0]]
    downs = [down_weight[0]]
    fin = [adapter_input_factors.reshape(-1, width)]
    fup = [adapter_output_factors.reshape(-1, hidden)]
    for r in range(1, stores):
        ups.append(swap(ups[0], "store", r))
        downs.append(swap(downs[0], "store", r))
        fin.append(swap(fin[0], "store", r))
        fup.append(swap(fup[0], "store", r))

    for d in range(1, outer):
        rows_of.append(
            call(
                functools.partial(pack_body, top, rows, width),
                [packed] * INNER,
                [[scal], *blocks[d]],
                move_flops,
                move_bytes,
            )
        )
    arrived = [[r[0]] + [swap(r[q], "inner", q) for q in range(1, INNER)] for r in rows_of]

    backs = []
    for d in range(outer):
        parts = column_parts(d, outer)
        kernel = pl.pallas_call(
            functools.partial(expert_body, top, rows, stores, parts),
            out_shape=[jax.ShapeDtypeStruct((rows, width // parts), BF16)] * (INNER * parts),
            in_specs=[SMEM] * 2 + [VMEM] * (INNER + 4 * stores),
            out_specs=[VMEM] * (INNER * parts),
            scratch_shapes=[
                pltpu.VMEM((INNER * rows, wide), BF16),
                pltpu.VMEM((stores * fin[0].shape[0], width), BF16),
                pltpu.VMEM((stores * fin[0].shape[0], hidden), BF16),
                pltpu.VMEM((INNER * rows, width), BF16),
            ],
            compiler_params=pltpu.CompilerParams(vmem_limit_bytes=28 * 1024 * 1024),
            cost_estimate=pl.CostEstimate(
                flops=2 * INNER * rows * width * hidden * 3, bytes_accessed=6 * width * hidden, transcendentals=0
            ),
            name="expert",
        )
        got = kernel(scal, adapted[:, 0], *arrived[d], *ups, *downs, *fin, *fup)
        backs.append([[got[i]] + [swap(got[q * parts + i], "inner", q) for q in range(1, INNER)] for i in range(parts)])

    def joining(d, steps):
        return [[swap(p, "outer", step) for p in partial(d + step)] for step in steps]

    def partial(d):
        more = joining(d, [1 << bit for bit in range(outer.bit_length()) if 1 << bit < lowest(d)])
        sums = []
        for i, rows_back in enumerate(backs[d]):
            sums.append(
                call(
                    functools.partial(partial_body, top, rows, width, len(blocks[d])),
                    jax.ShapeDtypeStruct((tok, width // len(backs[d])), BF16),
                    [[scal], *blocks[d], *rows_back, *(m[i] for m in more)],
                    move_flops,
                    move_bytes,
                )
            )
        return sums

    others = joining(0, [1 << bit for bit in range(outer.bit_length()) if 1 << bit < outer])
    return call(
        functools.partial(final_body, top, rows, width, [len(other) for other in others]),
        sums,
        [[scal], first[0]] + backs[0][0] + sum(others, []),
        move_flops,
        move_bytes,
    )


def solution(mesh):
    owners, stores = mesh.devices.shape
    grid = Mesh(mesh.devices.reshape(owners // INNER, INNER, stores), ("outer", "inner", "store"))
    expert, both = ("outer", "inner"), ("outer", "inner", "store")
    placed = (
        P(both, None),
        P(both, None),
        P(both, None),
        P(both),
        P(None, expert),
        P(expert, "store", None),
        P(expert, None, "store"),
        P("store", expert, None, None),
        P("store", expert, None, None),
    )

    return jax.shard_map(shards, mesh=grid, in_specs=placed, out_specs=P(both, None), check_vma=False)
```

```python
import functools

import jax
import jax.numpy as jnp
from jax import lax
from jax.experimental import pallas as pl
from jax.experimental.pallas import tpu as pltpu
from jax.sharding import Mesh, PartitionSpec as P


F32 = jnp.float32
BF16 = jnp.bfloat16
LANES = 128
INNER = 4
VMEM = pl.BlockSpec(memory_space=pltpu.VMEM)
SMEM = pl.BlockSpec(memory_space=pltpu.SMEM)


def call(body, outs, ins, flops, cost_bytes):
    smem = ins[0]
    return pl.pallas_call(
        body,
        out_shape=outs,
        in_specs=[SMEM] * len(smem) + [VMEM] * (len(ins) - 1),
        out_specs=jax.tree.map(lambda _: VMEM, outs),
        compiler_params=pltpu.CompilerParams(vmem_limit_bytes=20 * 1024 * 1024),
        cost_estimate=pl.CostEstimate(flops=flops, bytes_accessed=cost_bytes, transcendentals=0),
    )(*smem, *ins[1:])


def iota(shape, dim):
    return lax.broadcasted_iota(jnp.int32, shape, dim)


def packing(meta, expert, top):
    tok = meta.shape[0]
    lane = iota(meta.shape, 1)
    chosen = jnp.where(lane < top, meta, -1.0)
    named = jnp.zeros(meta.shape, F32)
    hits = []
    for q in range(INNER):
        target = lax.bitwise_xor(expert, q).astype(F32)
        hit = jnp.max(jnp.where(chosen == target, 1.0, 0.0), axis=1, keepdims=True)
        hits.append(hit)
        named = jnp.where(lane == q, hit, named)
    below = jnp.where(iota((tok, tok), 1) < iota((tok, tok), 0), 1.0, 0.0).astype(BF16)
    place = jnp.dot(below, named.astype(BF16), preferred_element_type=F32)
    slots = []
    for q in range(INNER):
        slot = jnp.where(hits[q] > 0.0, place[:, q : q + 1], -1.0)
        slots.append(slot)
    return slots


def one_hot(slots, rows):
    tok = slots[0].shape[0]
    lane = iota((tok, INNER * rows), 1).astype(F32)
    picked = jnp.zeros((tok, INNER * rows), F32)
    for q in range(INNER):
        at = jnp.where(slots[q] >= 0.0, slots[q] + float(q * rows), -1.0)
        picked = jnp.where(lane == at, 1.0, picked)
    return picked.astype(BF16)


def pack_rows(slots, wide, meta_t, outs, top, rows):
    tok, width = wide.shape[0], wide.shape[1] - LANES
    got = lax.dot_general(
        one_hot(slots, rows), wide[:, :width], (((0,), (0,)), ((), ())), preferred_element_type=F32
    ).astype(BF16)
    tenant = meta_t[top : top + 8].astype(BF16)
    lane = iota((tok, LANES), 1).astype(F32)
    for q in range(INNER):
        for c in range(width // LANES):
            outs[q][c * rows : (c + 1) * rows] = got[q * rows : (q + 1) * rows, c * LANES : (c + 1) * LANES]
        picked = jnp.where(lane == slots[q], 1.0, 0.0).astype(BF16)
        outs[q][width // LANES * rows :] = jnp.dot(tenant, picked, preferred_element_type=F32).astype(BF16)


def first_body(top, rows, expert_ref, tok_any, meta_ref, ext_ref, *refs):
    outs, sem = refs[:INNER], refs[INNER]
    tok, width = tok_any.shape
    copy = pltpu.make_async_copy(tok_any, ext_ref.at[:, pl.ds(0, width)], sem)
    copy.start()
    logits = meta_ref[top + 8 :]
    share = logits / jnp.sum(logits, axis=0, keepdims=True)
    high = share.astype(BF16).astype(F32)
    mid = (share - high).astype(BF16).astype(F32)
    low = share - high - mid
    pad = jnp.zeros((32 - top, tok), F32)
    meta_t = jnp.concatenate(
        [
            meta_ref[: top + 8],
            jnp.zeros((32 - top - 8, tok), F32),
            high,
            pad,
            mid,
            pad,
            low,
            pad,
        ],
        axis=0,
    )
    meta = meta_t.T
    ext_ref[:, width:] = meta.astype(BF16)
    slots = packing(meta, expert_ref[0], top)
    copy.wait()
    pack_rows(slots, ext_ref[...], meta_t, outs, top, rows)


def pack_body(top, rows, width, scal_ref, *refs):
    wide = either(scal_ref, refs[:-INNER])
    meta = wide[:, width:].astype(F32)
    pack_rows(packing(meta, scal_ref[0], top), wide, meta.T, refs[-INNER:], top, rows)


def expert_body(rows, stores, parts, scal_ref, adapted_ref, *refs):
    xs, refs = refs[:INNER], refs[INNER:]
    ups, refs = refs[:stores], refs[stores:]
    downs, refs = refs[:stores], refs[stores:]
    fins, refs = refs[:stores], refs[stores:]
    fups, refs = refs[:stores], refs[stores:]
    outs, (x_ref, fin_ref, fup_ref, y_ref) = refs[: INNER * parts], refs[INNER * parts :]
    store = scal_ref[1]
    width = ups[0].shape[0] * stores
    hidden = downs[0].shape[0]
    codes = []
    for q in range(INNER):
        for c in range(width // LANES):
            x_ref[q * rows : (q + 1) * rows, c * LANES : (c + 1) * LANES] = xs[q][c * rows : (c + 1) * rows]
        codes.append(xs[q][width // LANES * rows :].astype(F32).T[:rows, :1])
    code = jnp.concatenate(codes, axis=0)
    k = ups[0].shape[0]
    pre = None
    for r in range(stores):
        at = pl.multiple_of(lax.bitwise_xor(store, r) * k, LANES)
        part = jnp.dot(x_ref[:, pl.ds(at, k)], ups[r][...], preferred_element_type=F32)
        pre = part if pre is None else pre + part
    tenants = adapted_ref.shape[0]
    held = tenants // stores
    part = fins[0].shape[0]
    rank = part // held
    for r in range(stores):
        fin_ref[r * part : (r + 1) * part] = fins[r][...]
        fup_ref[r * part : (r + 1) * part] = fups[r][...]
    lane = iota((1, stores * part), 1)
    half = (lane % rank) < rank // 2
    tenant = lax.bitwise_xor(store, lane // part) * held + (lane // rank) % held
    allowed = jnp.zeros(lane.shape, F32)
    for u in range(tenants):
        allowed = jnp.where(tenant == u, adapted_ref[u].astype(F32), allowed)
    low = lax.dot_general(
        x_ref[...], fin_ref[...], (((1,), (1,)), ((), ())), preferred_element_type=F32
    )
    low = (low * jnp.where(code == tenant.astype(F32), allowed, 0.0)).astype(BF16)
    zero = jnp.zeros_like(low)
    gate = pre[:, :hidden] + jnp.dot(jnp.where(half, low, zero), fup_ref[...], preferred_element_type=F32)
    up = pre[:, hidden:] + jnp.dot(jnp.where(half, zero, low), fup_ref[...], preferred_element_type=F32)
    act = (gate / (1.0 + jnp.exp(-gate)) * up).astype(BF16)
    n = downs[0].shape[1]
    for r in range(stores):
        at = pl.multiple_of(lax.bitwise_xor(store, r) * n, LANES)
        y_ref[:, pl.ds(at, n)] = jnp.dot(act, downs[r][...], preferred_element_type=F32).astype(BF16)
    each = width // parts
    for q in range(INNER):
        for i in range(parts):
            outs[q * parts + i][...] = y_ref[q * rows : (q + 1) * rows, i * each : (i + 1) * each]


def weighted(expert, meta, ys, top, rows):
    slots = packing(meta, expert, top)
    lane = iota(meta.shape, 1)
    chosen = jnp.where(lane < top, meta, -1.0)
    share = sum(pltpu.roll(meta, LANES - 32 * (i + 1), 1) for i in range(3))
    total = None
    for q in range(INNER):
        target = lax.bitwise_xor(expert, q).astype(F32)
        mine = jnp.sum(jnp.where(chosen == target, share, 0.0), axis=1, keepdims=True)
        spot = iota((meta.shape[0], rows), 1).astype(F32)
        spread = jnp.where(spot == slots[q], 1.0, 0.0).astype(BF16)
        part = jnp.dot(spread, ys[q][...], preferred_element_type=F32) * mine
        total = part if total is None else total + part
    return total


def partial_body(top, rows, width, held, scal_ref, *refs):
    meta = either(scal_ref, refs[:held], slice(width, None)).astype(F32)
    refs = refs[held:]
    total = weighted(scal_ref[0], meta, refs[:INNER], top, rows)
    for other in refs[INNER:-1]:
        total = total + other[...].astype(F32)
    refs[-1][...] = total.astype(BF16)


def final_body(top, rows, width, splits, scal_ref, ext_ref, *refs):
    total = weighted(scal_ref[0], ext_ref[:, width:].astype(F32), refs[:INNER], top, rows)
    others, out = list(refs[INNER:-1]), refs[-1]
    for count in splits:
        pieces = [others.pop(0)[...].astype(F32) for _ in range(count)]
        total = total + (pieces[0] if count == 1 else jnp.concatenate(pieces, axis=1))
    out[...] = total.astype(BF16)


def swap(array, axis, distance):
    return lax.ppermute(array, axis, [(i, i ^ distance) for i in range(lax.axis_size(axis))])


def relayed(block):
    def send(array, pairs):
        return lax.ppermute(array, "outer", pairs)

    middle, outward = [(1, 2), (2, 1)], [(1, 0), (2, 3)]
    near = swap(block, "outer", 1)
    over = send(block, middle)
    over_near = send(near, middle)
    end_over = send(over, outward)
    end_over_near = send(over_near, outward)
    return [(block,), (near,), (over_near, end_over), (over, end_over_near)]


def either(scal_ref, block_refs, columns=slice(None)):
    if len(block_refs) == 1:
        return block_refs[0][:, columns]
    return jnp.where(scal_ref[2] > 0, block_refs[1][:, columns], block_refs[0][:, columns])


def lowest(d):
    return d & -d


def column_parts(d, outer):
    return 2 if outer == 4 and d in (2, 3) else 1


def shards(
    tokens,
    chosen_expert_index,
    router_weight_logits,
    token_tenant_index,
    adapted,
    gate_up_weight,
    down_weight,
    adapter_input_factors,
    adapter_output_factors,
):
    tok, width = tokens.shape
    top = chosen_expert_index.shape[1]
    outer, stores = lax.axis_size("outer"), lax.axis_size("store")
    owners = outer * INNER
    cap = max(2, tok * top * 9 // (8 * owners))
    rows = -(-cap // 8) * 8
    hidden = down_weight.shape[1]
    wide = width + LANES
    expert = lax.axis_index("outer") * INNER + lax.axis_index("inner")
    store = lax.axis_index("store")
    place = lax.axis_index("outer")
    ends = jnp.logical_or(place == 0, place == outer - 1)
    scal = jnp.stack([expert, store, ends.astype(jnp.int32)]).astype(jnp.int32)
    packed = jax.ShapeDtypeStruct((width // LANES * rows + 8, LANES), BF16)
    ext_shape = jax.ShapeDtypeStruct((tok, wide), BF16)
    sums = jax.ShapeDtypeStruct((tok, width), BF16)

    move_flops = 2 * tok * INNER * rows * width
    move_bytes = 2 * (tok + INNER * rows) * wide
    ints = jnp.pad(chosen_expert_index.T, ((0, top + 8), (0, 0)))
    ints = ints + jnp.pad(token_tenant_index.reshape(1, -1), ((top, top + 7), (0, 0)))
    meta = ints.astype(F32) + jnp.pad(router_weight_logits.T, ((top + 8, 0), (0, 0)))
    first = pl.pallas_call(
        functools.partial(first_body, top, rows),
        out_shape=[ext_shape] + [packed] * INNER,
        in_specs=[SMEM, pl.BlockSpec(memory_space=pl.ANY), VMEM],
        out_specs=[VMEM] * (1 + INNER),
        scratch_shapes=[pltpu.SemaphoreType.DMA],
        compiler_params=pltpu.CompilerParams(vmem_limit_bytes=20 * 1024 * 1024),
        cost_estimate=pl.CostEstimate(flops=move_flops, bytes_accessed=move_bytes, transcendentals=0),
        name="first",
    )(scal, tokens, meta)
    if outer == 4:
        blocks = relayed(first[0])
    else:
        blocks = [(first[0],)]
        for d in range(1, outer):
            blocks.append((swap(blocks[d - lowest(d)][0], "outer", lowest(d)),))
    rows_of = [first[1:]]

    ups = [gate_up_weight[0]]
    downs = [down_weight[0]]
    fin = [adapter_input_factors.reshape(-1, width)]
    fup = [adapter_output_factors.reshape(-1, hidden)]
    for r in range(1, stores):
        ups.append(swap(ups[0], "store", r))
        downs.append(swap(downs[0], "store", r))
        fin.append(swap(fin[0], "store", r))
        fup.append(swap(fup[0], "store", r))

    for d in range(1, outer):
        rows_of.append(
            call(
                functools.partial(pack_body, top, rows, width),
                [packed] * INNER,
                [[scal], *blocks[d]],
                move_flops,
                move_bytes,
            )
        )
    arrived = [[r[0]] + [swap(r[q], "inner", q) for q in range(1, INNER)] for r in rows_of]

    backs = []
    for d in range(outer):
        parts = column_parts(d, outer)
        kernel = pl.pallas_call(
            functools.partial(expert_body, rows, stores, parts),
            out_shape=[jax.ShapeDtypeStruct((rows, width // parts), BF16)] * (INNER * parts),
            in_specs=[SMEM] * 2 + [VMEM] * (INNER + 4 * stores),
            out_specs=[VMEM] * (INNER * parts),
            scratch_shapes=[
                pltpu.VMEM((INNER * rows, width), BF16),
                pltpu.VMEM((stores * fin[0].shape[0], width), BF16),
                pltpu.VMEM((stores * fin[0].shape[0], hidden), BF16),
                pltpu.VMEM((INNER * rows, width), BF16),
            ],
            compiler_params=pltpu.CompilerParams(vmem_limit_bytes=28 * 1024 * 1024),
            cost_estimate=pl.CostEstimate(
                flops=2 * INNER * rows * width * hidden * 3, bytes_accessed=6 * width * hidden, transcendentals=0
            ),
            name="expert",
        )
        got = kernel(scal, adapted[:, 0], *arrived[d], *ups, *downs, *fin, *fup)
        backs.append([[got[i]] + [swap(got[q * parts + i], "inner", q) for q in range(1, INNER)] for i in range(parts)])

    def joining(d, steps):
        return [[swap(p, "outer", step) for p in partial(d + step)] for step in steps]

    def partial(d):
        more = joining(d, [1 << bit for bit in range(outer.bit_length()) if 1 << bit < lowest(d)])
        sums = []
        for i, rows_back in enumerate(backs[d]):
            sums.append(
                call(
                    functools.partial(partial_body, top, rows, width, len(blocks[d])),
                    jax.ShapeDtypeStruct((tok, width // len(backs[d])), BF16),
                    [[scal], *blocks[d], *rows_back, *(m[i] for m in more)],
                    move_flops,
                    move_bytes,
                )
            )
        return sums

    others = joining(0, [1 << bit for bit in range(outer.bit_length()) if 1 << bit < outer])
    return call(
        functools.partial(final_body, top, rows, width, [len(other) for other in others]),
        sums,
        [[scal], first[0]] + backs[0][0] + sum(others, []),
        move_flops,
        move_bytes,
    )


def solution(mesh):
    owners, stores = mesh.devices.shape
    grid = Mesh(mesh.devices.reshape(owners // INNER, INNER, stores), ("outer", "inner", "store"))
    expert, both = ("outer", "inner"), ("outer", "inner", "store")
    placed = (
        P(both, None),
        P(both, None),
        P(both, None),
        P(both),
        P(None, expert),
        P(expert, "store", None),
        P(expert, None, "store"),
        P("store", expert, None, None),
        P("store", expert, None, None),
    )

    return jax.shard_map(shards, mesh=grid, in_specs=placed, out_specs=P(both, None), check_vma=False)
```

```python
import functools

import jax
import jax.numpy as jnp
from jax import lax
from jax.experimental import pallas as pl
from jax.experimental.pallas import tpu as pltpu
from jax.sharding import Mesh, PartitionSpec as P


F32 = jnp.float32
BF16 = jnp.bfloat16
LANES = 128
INNER = 4
VMEM = pl.BlockSpec(memory_space=pltpu.VMEM)
SMEM = pl.BlockSpec(memory_space=pltpu.SMEM)


def call(body, outs, ins, flops, cost_bytes):
    smem = ins[0]
    return pl.pallas_call(
        body,
        out_shape=outs,
        in_specs=[SMEM] * len(smem) + [VMEM] * (len(ins) - 1),
        out_specs=jax.tree.map(lambda _: VMEM, outs),
        compiler_params=pltpu.CompilerParams(vmem_limit_bytes=20 * 1024 * 1024),
        cost_estimate=pl.CostEstimate(flops=flops, bytes_accessed=cost_bytes, transcendentals=0),
    )(*smem, *ins[1:])


def iota(shape, dim):
    return lax.broadcasted_iota(jnp.int32, shape, dim)


def packing(meta, expert, top):
    tok = meta.shape[0]
    lane = iota(meta.shape, 1)
    chosen = jnp.where(lane < top, meta, -1.0)
    named = jnp.zeros(meta.shape, F32)
    hits = []
    for q in range(INNER):
        target = lax.bitwise_xor(expert, q).astype(F32)
        hit = jnp.max(jnp.where(chosen == target, 1.0, 0.0), axis=1, keepdims=True)
        hits.append(hit)
        named = jnp.where(lane == q, hit, named)
    below = jnp.where(iota((tok, tok), 1) < iota((tok, tok), 0), 1.0, 0.0).astype(BF16)
    place = jnp.dot(below, named.astype(BF16), preferred_element_type=F32)
    slots = []
    for q in range(INNER):
        slot = jnp.where(hits[q] > 0.0, place[:, q : q + 1], -1.0)
        slots.append(slot)
    return slots


def one_hot(slots, rows):
    tok = slots[0].shape[0]
    lane = iota((tok, INNER * rows), 1).astype(F32)
    picked = jnp.zeros((tok, INNER * rows), F32)
    for q in range(INNER):
        at = jnp.where(slots[q] >= 0.0, slots[q] + float(q * rows), -1.0)
        picked = jnp.where(lane == at, 1.0, picked)
    return picked.astype(BF16)


def pack_rows(slots, wide, meta_t, outs, top, rows):
    tok, width = wide.shape[0], wide.shape[1] - LANES
    got = lax.dot_general(
        one_hot(slots, rows), wide[:, :width], (((0,), (0,)), ((), ())), preferred_element_type=F32
    ).astype(BF16)
    tenant = meta_t[top : top + 8].astype(BF16)
    lane = iota((tok, LANES), 1).astype(F32)
    for q in range(INNER):
        for c in range(width // LANES):
            outs[q][c * rows : (c + 1) * rows] = got[q * rows : (q + 1) * rows, c * LANES : (c + 1) * LANES]
        picked = jnp.where(lane == slots[q], 1.0, 0.0).astype(BF16)
        outs[q][width // LANES * rows :] = jnp.dot(tenant, picked, preferred_element_type=F32).astype(BF16)


def first_body(top, rows, expert_ref, tok_any, meta_ref, ext_ref, plan_ref, *refs):
    outs, sem = refs[:INNER], refs[INNER]
    tok, width = tok_any.shape
    copy = pltpu.make_async_copy(tok_any, ext_ref.at[:, pl.ds(0, width)], sem)
    copy.start()
    logits = meta_ref[top + 8 :]
    share = logits / jnp.sum(logits, axis=0, keepdims=True)
    high = share.astype(BF16).astype(F32)
    mid = (share - high).astype(BF16).astype(F32)
    low = share - high - mid
    pad = jnp.zeros((32 - top, tok), F32)
    meta_t = jnp.concatenate(
        [
            meta_ref[: top + 8],
            jnp.zeros((32 - top - 8, tok), F32),
            high,
            pad,
            mid,
            pad,
            low,
            pad,
        ],
        axis=0,
    )
    meta = meta_t.T
    ext_ref[:, width:] = meta.astype(BF16)
    slots = packing(meta, expert_ref[0], top)
    copy.wait()
    pack_rows(slots, ext_ref[...], meta_t, outs, top, rows)
    plan_ref[...] = plan_of(slots, meta, expert_ref[0], top)


def pack_body(top, rows, width, scal_ref, *refs):
    wide = either(scal_ref, refs[: -INNER - 1])
    meta = wide[:, width:].astype(F32)
    slots = packing(meta, scal_ref[0], top)
    pack_rows(slots, wide, meta.T, refs[-INNER:], top, rows)
    refs[-INNER - 1][...] = plan_of(slots, meta, scal_ref[0], top)


def expert_body(rows, stores, parts, scal_ref, adapted_ref, *refs):
    xs, refs = refs[:INNER], refs[INNER:]
    ups, refs = refs[:stores], refs[stores:]
    downs, refs = refs[:stores], refs[stores:]
    fins, refs = refs[:stores], refs[stores:]
    fups, refs = refs[:stores], refs[stores:]
    outs, (x_ref, fin_ref, fup_ref, y_ref) = refs[: INNER * parts], refs[INNER * parts :]
    store = scal_ref[1]
    width = ups[0].shape[0] * stores
    hidden = downs[0].shape[0]
    codes = []
    for q in range(INNER):
        for c in range(width // LANES):
            x_ref[q * rows : (q + 1) * rows, c * LANES : (c + 1) * LANES] = xs[q][c * rows : (c + 1) * rows]
        codes.append(xs[q][width // LANES * rows :].astype(F32).T[:rows, :1])
    code = jnp.concatenate(codes, axis=0)
    k = ups[0].shape[0]
    pre = None
    for r in range(stores):
        at = pl.multiple_of(lax.bitwise_xor(store, r) * k, LANES)
        part = jnp.dot(x_ref[:, pl.ds(at, k)], ups[r][...], preferred_element_type=F32)
        pre = part if pre is None else pre + part
    tenants = adapted_ref.shape[0]
    held = tenants // stores
    part = fins[0].shape[0]
    rank = part // held
    for r in range(stores):
        fin_ref[r * part : (r + 1) * part] = fins[r][...]
        fup_ref[r * part : (r + 1) * part] = fups[r][...]
    lane = iota((1, stores * part), 1)
    half = (lane % rank) < rank // 2
    tenant = lax.bitwise_xor(store, lane // part) * held + (lane // rank) % held
    allowed = jnp.zeros(lane.shape, F32)
    for u in range(tenants):
        allowed = jnp.where(tenant == u, adapted_ref[u].astype(F32), allowed)
    low = lax.dot_general(
        x_ref[...], fin_ref[...], (((1,), (1,)), ((), ())), preferred_element_type=F32
    )
    low = (low * jnp.where(code == tenant.astype(F32), allowed, 0.0)).astype(BF16)
    zero = jnp.zeros_like(low)
    gate = pre[:, :hidden] + jnp.dot(jnp.where(half, low, zero), fup_ref[...], preferred_element_type=F32)
    up = pre[:, hidden:] + jnp.dot(jnp.where(half, zero, low), fup_ref[...], preferred_element_type=F32)
    act = (gate / (1.0 + jnp.exp(-gate)) * up).astype(BF16)
    n = downs[0].shape[1]
    for r in range(stores):
        at = pl.multiple_of(lax.bitwise_xor(store, r) * n, LANES)
        y_ref[:, pl.ds(at, n)] = jnp.dot(act, downs[r][...], preferred_element_type=F32).astype(BF16)
    each = width // parts
    for q in range(INNER):
        for i in range(parts):
            outs[q * parts + i][...] = y_ref[q * rows : (q + 1) * rows, i * each : (i + 1) * each]


def plan_of(slots, meta, expert, top):
    lane = iota(meta.shape, 1)
    chosen = jnp.where(lane < top, meta, -1.0)
    share = sum(pltpu.roll(meta, LANES - 32 * (i + 1), 1) for i in range(3))
    plan = jnp.zeros(meta.shape, F32)
    for q in range(INNER):
        target = lax.bitwise_xor(expert, q).astype(F32)
        mine = jnp.sum(jnp.where(chosen == target, share, 0.0), axis=1, keepdims=True)
        plan = jnp.where(lane == q, slots[q], plan)
        plan = jnp.where(lane == INNER + q, mine, plan)
    return plan


def weighted(plan, ys, rows):
    spot = iota((plan.shape[0], rows), 1).astype(F32)
    total = None
    for q in range(INNER):
        spread = jnp.where(spot == plan[:, q : q + 1], 1.0, 0.0).astype(BF16)
        part = jnp.dot(spread, ys[q][...], preferred_element_type=F32) * plan[:, INNER + q : INNER + q + 1]
        total = part if total is None else total + part
    return total


def sum_body(rows, plan_ref, *refs):
    total = weighted(plan_ref[...], refs[:INNER], rows)
    for other in refs[INNER:-1]:
        total = total + other[...].astype(F32)
    refs[-1][...] = total.astype(refs[-1].dtype)


def final_body(splits, total_ref, *refs):
    total = total_ref[...]
    others, out = list(refs[:-1]), refs[-1]
    for count in splits:
        pieces = [others.pop(0)[...].astype(F32) for _ in range(count)]
        total = total + (pieces[0] if count == 1 else jnp.concatenate(pieces, axis=1))
    out[...] = total.astype(BF16)


def swap(array, axis, distance):
    return lax.ppermute(array, axis, [(i, i ^ distance) for i in range(lax.axis_size(axis))])


def relayed(block):
    def send(array, pairs):
        return lax.ppermute(array, "outer", pairs)

    middle, outward = [(1, 2), (2, 1)], [(1, 0), (2, 3)]
    near = swap(block, "outer", 1)
    over = send(block, middle)
    over_near = send(near, middle)
    end_over = send(over, outward)
    end_over_near = send(over_near, outward)
    return [(block,), (near,), (over_near, end_over), (over, end_over_near)]


def either(scal_ref, block_refs, columns=slice(None)):
    if len(block_refs) == 1:
        return block_refs[0][:, columns]
    return jnp.where(scal_ref[2] > 0, block_refs[1][:, columns], block_refs[0][:, columns])


def lowest(d):
    return d & -d


def column_parts(d, outer):
    return 2 if outer == 4 and d in (2, 3) else 1


def shards(
    tokens,
    chosen_expert_index,
    router_weight_logits,
    token_tenant_index,
    adapted,
    gate_up_weight,
    down_weight,
    adapter_input_factors,
    adapter_output_factors,
):
    tok, width = tokens.shape
    top = chosen_expert_index.shape[1]
    outer, stores = lax.axis_size("outer"), lax.axis_size("store")
    owners = outer * INNER
    cap = max(2, tok * top * 9 // (8 * owners))
    rows = -(-cap // 8) * 8
    hidden = down_weight.shape[1]
    wide = width + LANES
    expert = lax.axis_index("outer") * INNER + lax.axis_index("inner")
    store = lax.axis_index("store")
    place = lax.axis_index("outer")
    ends = jnp.logical_or(place == 0, place == outer - 1)
    scal = jnp.stack([expert, store, ends.astype(jnp.int32)]).astype(jnp.int32)
    packed = jax.ShapeDtypeStruct((width // LANES * rows + 8, LANES), BF16)
    plan_shape = jax.ShapeDtypeStruct((tok, LANES), F32)
    ext_shape = jax.ShapeDtypeStruct((tok, wide), BF16)
    sums = jax.ShapeDtypeStruct((tok, width), BF16)

    move_flops = 2 * tok * INNER * rows * width
    move_bytes = 2 * (tok + INNER * rows) * wide
    ints = jnp.pad(chosen_expert_index.T, ((0, top + 8), (0, 0)))
    ints = ints + jnp.pad(token_tenant_index.reshape(1, -1), ((top, top + 7), (0, 0)))
    meta = ints.astype(F32) + jnp.pad(router_weight_logits.T, ((top + 8, 0), (0, 0)))
    first = pl.pallas_call(
        functools.partial(first_body, top, rows),
        out_shape=[ext_shape, plan_shape] + [packed] * INNER,
        in_specs=[SMEM, pl.BlockSpec(memory_space=pl.ANY), VMEM],
        out_specs=[VMEM] * (2 + INNER),
        scratch_shapes=[pltpu.SemaphoreType.DMA],
        compiler_params=pltpu.CompilerParams(vmem_limit_bytes=20 * 1024 * 1024),
        cost_estimate=pl.CostEstimate(flops=move_flops, bytes_accessed=move_bytes, transcendentals=0),
        name="first",
    )(scal, tokens, meta)
    if outer == 4:
        blocks = relayed(first[0])
    else:
        blocks = [(first[0],)]
        for d in range(1, outer):
            blocks.append((swap(blocks[d - lowest(d)][0], "outer", lowest(d)),))
    plans, rows_of = [first[1]], [first[2:]]

    ups = [gate_up_weight[0]]
    downs = [down_weight[0]]
    fin = [adapter_input_factors.reshape(-1, width)]
    fup = [adapter_output_factors.reshape(-1, hidden)]
    for r in range(1, stores):
        ups.append(swap(ups[0], "store", r))
        downs.append(swap(downs[0], "store", r))
        fin.append(swap(fin[0], "store", r))
        fup.append(swap(fup[0], "store", r))

    for d in range(1, outer):
        got = call(
            functools.partial(pack_body, top, rows, width),
            [plan_shape] + [packed] * INNER,
            [[scal], *blocks[d]],
            move_flops,
            move_bytes,
        )
        plans.append(got[0])
        rows_of.append(got[1:])
    arrived = [[r[0]] + [swap(r[q], "inner", q) for q in range(1, INNER)] for r in rows_of]

    backs = []
    for d in range(outer):
        parts = column_parts(d, outer)
        kernel = pl.pallas_call(
            functools.partial(expert_body, rows, stores, parts),
            out_shape=[jax.ShapeDtypeStruct((rows, width // parts), BF16)] * (INNER * parts),
            in_specs=[SMEM] * 2 + [VMEM] * (INNER + 4 * stores),
            out_specs=[VMEM] * (INNER * parts),
            scratch_shapes=[
                pltpu.VMEM((INNER * rows, width), BF16),
                pltpu.VMEM((stores * fin[0].shape[0], width), BF16),
                pltpu.VMEM((stores * fin[0].shape[0], hidden), BF16),
                pltpu.VMEM((INNER * rows, width), BF16),
            ],
            compiler_params=pltpu.CompilerParams(vmem_limit_bytes=28 * 1024 * 1024),
            cost_estimate=pl.CostEstimate(
                flops=2 * INNER * rows * width * hidden * 3, bytes_accessed=6 * width * hidden, transcendentals=0
            ),
            name="expert",
        )
        got = kernel(scal, adapted[:, 0], *arrived[d], *ups, *downs, *fin, *fup)
        backs.append([[got[i]] + [swap(got[q * parts + i], "inner", q) for q in range(1, INNER)] for i in range(parts)])

    def joining(d, steps):
        return [[swap(p, "outer", step) for p in partial(d + step)] for step in steps]

    def partial(d):
        more = joining(d, [1 << bit for bit in range(outer.bit_length()) if 1 << bit < lowest(d)])
        sums = []
        for i, rows_back in enumerate(backs[d]):
            sums.append(
                call(
                    functools.partial(sum_body, rows),
                    jax.ShapeDtypeStruct((tok, width // len(backs[d])), BF16),
                    [[], plans[d], *rows_back, *(m[i] for m in more)],
                    move_flops,
                    move_bytes,
                )
            )
        return sums

    others = joining(0, [1 << bit for bit in range(outer.bit_length()) if 1 << bit < outer])
    own = call(
        functools.partial(sum_body, rows),
        jax.ShapeDtypeStruct((tok, width), F32),
        [[], plans[0], *backs[0][0]],
        move_flops,
        move_bytes,
    )
    return call(
        functools.partial(final_body, [len(other) for other in others]),
        sums,
        [[], own] + sum(others, []),
        tok * width,
        8 * tok * width,
    )


def solution(mesh):
    owners, stores = mesh.devices.shape
    grid = Mesh(mesh.devices.reshape(owners // INNER, INNER, stores), ("outer", "inner", "store"))
    expert, both = ("outer", "inner"), ("outer", "inner", "store")
    placed = (
        P(both, None),
        P(both, None),
        P(both, None),
        P(both),
        P(None, expert),
        P(expert, "store", None),
        P(expert, None, "store"),
        P("store", expert, None, None),
        P("store", expert, None, None),
    )

    return jax.shard_map(shards, mesh=grid, in_specs=placed, out_specs=P(both, None), check_vma=False)
```
